512 devices in a mesh: section: 8 (over z), expert: 16 (over y, core), dp: 4 (over x).
Axes of the slice: x: 4, y: 8, z: 8, core: 2. Of those that a mesh axis runs over, the one named last changes fastest.
Arguments:
- arrivals: bfloat16 [8, 4096, 2048], P('section', ('expert', 'dp')), may hold values from -6 to 6
- fresh: bfloat16 [1, 4096, 2048], P(None, ('expert', 'dp')), may hold values from -6 to 6
- routes: int32 [8, 2, 4096, 6], P('section', None, ('expert', 'dp')), may hold values from 0 to 63, as said below
- gates: bfloat16 [8, 2, 4096, 6], P('section', None, ('expert', 'dp')), may hold values from 0.099609375 to 1
- cotangent: bfloat16 [8, 2, 4096, 2048], P('section', None, ('expert', 'dp')), may hold values from -0.3125 to 0.3125
- norm_gain: float32 [8, 2048], P('section'), may hold values from 0.5 to 1.5
- w_gate: bfloat16 [8, 5632, 2048], P('section', 'expert', 'dp'), may hold values from -0.125 to 0.125
- w_up: bfloat16 [8, 5632, 2048], P('section', 'expert', 'dp'), may hold values from -0.125 to 0.125
- w_down: bfloat16 [8, 5632, 2048], P('section', 'expert', 'dp'), may hold values from -0.15625 to 0.15625
Outputs:
- layer_out: bfloat16 [8, 2, 4096, 2048], P('section', None, ('expert', 'dp'))
- grad_down: float32 [8, 5632, 2048], P('section', 'expert', 'dp')
The draws below stay inside these ranges and needn't reach their ends.
Inputs may be any that keep to these rules, and one draw needn't show every extreme that they name: `routes`: each token's 6 entries are different expert numbers.
All inputs are finite; a program needn't handle non-finite values.
Results may differ from the reference program's by a relative error of at most 0.0085.
Values may be sent and summed in bfloat16 or wider, within the bound.
No kernel may reach another device: no remote copies, remote signals or barrier semaphores. Data moves between devices by JAX's collectives and lax.ppermute only.
A program may use at most 64 MiB of HBM per device.

```python
import jax
import jax.numpy as jnp
from jax import lax

D = 2048
EXPERTS = 64
TOPK = 6
EXP_HID = 1408
SPLIT = 4
CAP = 12
STEPS = 2
TOK_MB = 64
FLIGHT = 4
HID_DEV = 352
LAYERS = 8
FRESH = 1
TOKENS = 4096


def draw_routes(key, part):
    total_rows = LAYERS * STEPS * TOKENS
    groups = LAYERS * STEPS
    blocks = total_rows // TOK_MB
    key_noise, key_hot, key_rank, key_pick, key_boost = jax.random.split(jax.random.fold_in(key, 7), 5)
    column = jnp.arange(EXPERTS, dtype=jnp.int32)
    noise = jax.random.randint(key_noise, (total_rows, EXPERTS), 0, 1 << 20, dtype=jnp.int32)
    scores = noise * EXPERTS + column[None, :]
    hottest = jax.random.randint(key_hot, (groups,), 0, FLIGHT, dtype=jnp.int32)
    hot_rows = jnp.repeat(hottest, TOKENS)
    ranking = jax.random.randint(key_rank, (blocks, TOK_MB), 0, 1 << 20, dtype=jnp.int32) * TOK_MB + jnp.arange(TOK_MB, dtype=jnp.int32)[None, :]
    ordering = jnp.argsort(jnp.argsort(ranking, axis=1), axis=1).reshape(total_rows)
    forced = (ordering < CAP).astype(jnp.int32)
    scores = scores + forced[:, None] * (column[None, :] == hot_rows[:, None]).astype(jnp.int32) * (1 << 28)
    picked = jax.random.randint(key_pick, (total_rows,), 0, FLIGHT, dtype=jnp.int32)
    boosted = (jax.random.randint(key_boost, (total_rows,), 0, 4, dtype=jnp.int32) == 0).astype(jnp.int32)
    scores = scores + boosted[:, None] * (column[None, :] == picked[:, None]).astype(jnp.int32) * (1 << 27)
    top_values, chosen = lax.top_k(scores, TOPK)
    return chosen.astype(jnp.int32).reshape(LAYERS, STEPS, TOKENS, TOPK)


def level_of(own_key, dims, shards, low, largest):
    level = 1.0
    for dim, blocks in shards:
        draws = jax.random.uniform(jax.random.fold_in(jax.random.fold_in(own_key, 6), dim), (blocks,), jnp.float32, low / len(shards), largest / len(shards))
        level = level * jnp.repeat(jnp.exp(draws), dims[dim] // blocks).reshape((-1,) + (1,) * (len(dims) - 1 - dim))
    return level


def gaussian(rng, extent, width, bound, cuts=(), kind=jnp.bfloat16):
    level = level_of(rng, extent, cuts, -0.22, 0.18) if cuts else 1.0
    values = jax.random.normal(rng, extent, jnp.float32) * width * level
    return jnp.minimum(jnp.maximum(values, -bound), bound).astype(kind)


def setup_inputs(seed: int = 0) -> dict:
    seeds = jax.random.split(jax.random.key(seed), 10)
    return {
        "arrivals": gaussian(seeds[0], (LAYERS, TOKENS, D), 1.0, 6.0, ((0, 8), (1, 64))),
        "fresh": gaussian(seeds[1], (FRESH, TOKENS, D), 1.0, 6.0, ((1, 64),)),
        "routes": draw_routes(jax.random.fold_in(seeds[9], 71), 0),
        "gates": jnp.clip(0.099609375 + 0.9003906 * jax.random.uniform(seeds[3], (LAYERS, STEPS, TOKENS, TOPK), jnp.float32) ** level_of(seeds[3], (LAYERS, STEPS, TOKENS, TOPK), ((0, 8), (2, 64)), -0.2, 0.2), 0.099609375, 1.0).astype(jnp.bfloat16),
        "cotangent": gaussian(seeds[4], (LAYERS, STEPS, TOKENS, D), 0.05, 0.3125, ((0, 8), (2, 64))),
        "norm_gain": jnp.clip(1.0 + 0.1 * jax.random.normal(seeds[5], (LAYERS, D), jnp.float32), 0.5, 1.5),
        "w_gate": gaussian(seeds[6], (LAYERS, FLIGHT * EXP_HID, D), D ** -0.5, 0.125, ((0, 8), (1, 16), (2, 4))),
        "w_up": gaussian(seeds[7], (LAYERS, FLIGHT * EXP_HID, D), D ** -0.5, 0.125, ((0, 8), (1, 16), (2, 4))),
        "w_down": gaussian(seeds[8], (LAYERS, FLIGHT * EXP_HID, D), EXP_HID ** -0.5, 0.15625, ((0, 8), (1, 16), (2, 4))),
    }


def rms_normed(values, gains):
    floats = values.astype(jnp.float32)
    scale = lax.rsqrt(lax.optimization_barrier(jnp.mean(floats * floats, axis=-1, keepdims=True)) + 0.5)
    return (floats * scale * gains[None, :]).astype(jnp.bfloat16)

def layer(inputs, routing, weights, cot, gains, gate_rows, up_rows, down_rows):
    highest = lax.Precision.HIGHEST
    blocks = TOKENS // TOK_MB
    normed = rms_normed(inputs, gains).astype(jnp.float32).reshape(blocks, TOK_MB, D)
    cot_blocks = cot.astype(jnp.float32).reshape(blocks, TOK_MB, D)
    route_blocks = routing.reshape(blocks, TOK_MB, TOPK)
    weight_blocks = weights.astype(jnp.float32).reshape(blocks, TOK_MB, TOPK)
    slot_ids = jnp.arange(CAP, dtype=jnp.int32)
    mixture = jnp.zeros((blocks, TOK_MB, D), jnp.float32)
    grads = []
    for expert in range(FLIGHT):
        matches = route_blocks == expert
        naming = jnp.any(matches, axis=-1).astype(jnp.int32)
        shares = lax.optimization_barrier(jnp.sum(jnp.where(matches, weight_blocks, 0.0), axis=-1))
        places = jnp.cumsum(naming, axis=1) - naming
        select = ((naming[:, None, :] == 1) & (places[:, None, :] == slot_ids[None, :, None])).astype(jnp.float32)
        rows_tok = jnp.einsum('bpt,btd->bpd', select, normed, precision=highest).reshape(blocks * CAP, D)
        rows_cot = jnp.einsum('bpt,btd->bpd', select, cot_blocks, precision=highest).reshape(blocks * CAP, D)
        rows_gate = jnp.einsum('bpt,bt->bp', select, shares, precision=highest)
        first_row = expert * EXP_HID
        gate_w = gate_rows[first_row:first_row + EXP_HID].astype(jnp.float32)
        up_w = up_rows[first_row:first_row + EXP_HID].astype(jnp.float32)
        down_w = down_rows[first_row:first_row + EXP_HID].astype(jnp.float32)
        gate_act = jnp.dot(rows_tok, gate_w.T, precision=highest)
        up_act = jnp.dot(rows_tok, up_w.T, precision=highest)
        hidden = lax.optimization_barrier((jax.nn.silu(gate_act) * up_act).astype(jnp.bfloat16)).astype(jnp.float32)
        pieces = jnp.einsum('rmf,mfd->rmd', hidden.reshape(blocks * CAP, SPLIT, HID_DEV), down_w.reshape(SPLIT, HID_DEV, D), precision=highest)
        pieces = lax.optimization_barrier(pieces.astype(jnp.bfloat16)).astype(jnp.float32)
        expert_out = lax.optimization_barrier(jnp.sum(pieces, axis=1)).reshape(blocks, CAP, D)
        mixture = mixture + jnp.einsum('bpt,bp,bpd->btd', select, rows_gate, expert_out, precision=highest)
        gate_flat = rows_gate.reshape(blocks * CAP)
        weighted = lax.optimization_barrier((hidden * gate_flat[:, None]).astype(jnp.bfloat16)).astype(jnp.float32)
        grads.append(jnp.dot(weighted.T, rows_cot, precision=highest))
    result = (inputs.astype(jnp.float32) + mixture.reshape(TOKENS, D)).astype(jnp.bfloat16)
    return (result, jnp.concatenate(grads, axis=0))

def reference(arrivals, fresh, routes, gates, cotangent, norm_gain, w_gate, w_up, w_down):
    results = []
    grads = []
    for layer_num in range(LAYERS):
        row_out = []
        total = jnp.zeros((FLIGHT * EXP_HID, D), jnp.float32)
        for turn_num in range(STEPS):
            if turn_num == 0:
                inputs = arrivals[layer_num]
            elif layer_num == 0:
                inputs = fresh[turn_num - 1]
            else:
                inputs = results[layer_num - 1][turn_num - 1]
            output, grad_part = layer(inputs, routes[layer_num, turn_num], gates[layer_num, turn_num], cotangent[layer_num, turn_num], norm_gain[layer_num], w_gate[layer_num], w_up[layer_num], w_down[layer_num])
            row_out.append(output)
            total = total + grad_part
        results.append(row_out)
        grads.append(total)
    layer_out = jnp.stack([jnp.stack(row_out) for row_out in results])
    grad_down = jnp.stack(grads)
    return (layer_out, grad_down)
```

```python
import functools

import jax
import jax.numpy as jnp
from jax import lax
from jax.experimental import pallas as pl
from jax.experimental.pallas import tpu as pltpu
from jax.sharding import PartitionSpec as P

SPLIT = 4
CAP = 12
VMEM = pltpu.MemorySpace.VMEM
SMEM = pltpu.MemorySpace.SMEM
F32 = jnp.float32
BF16 = jnp.bfloat16
NT = (((1,), (1,)), ((), ()))
TN = (((0,), (0,)), ((), ()))


def call(body, outs, scratch, *args):
    specs = [pl.BlockSpec(memory_space=SMEM)]
    specs += [pl.BlockSpec(memory_space=VMEM) for _ in args[1:]]
    many = isinstance(outs, (tuple, list))
    return pl.pallas_call(
        body,
        out_shape=outs,
        in_specs=specs,
        out_specs=[pl.BlockSpec(memory_space=VMEM) for _ in outs]
        if many
        else pl.BlockSpec(memory_space=VMEM),
        scratch_shapes=scratch,
        compiler_params=pltpu.CompilerParams(vmem_limit_bytes=48 * 1024 * 1024),
    )(*args)


def row_codes(rows, width):
    row = lax.broadcasted_iota(jnp.int32, (rows, width), 0)
    return row // (4 * CAP), (row // CAP) % 2, row % CAP


def by_expert(table, expert):
    out = table[3:4, :]
    for e in (2, 1, 0):
        out = jnp.where(expert == e, table[e : e + 1, :], out)
    return out


def block(shift, part, width):
    return pl.ds(pl.multiple_of(((shift + part) % 4) * width, width), width)


def pick(choice, first, second):
    return jnp.where(choice == 1, first, second)


def pack_kernel(use_second, meta, x_ref, y_ref, gain_ref, place_ref, out_ref, norm_ref):
    shift = meta[0]
    x = x_ref[...].astype(F32)
    if use_second:
        x = jnp.where(meta[2] == 1, y_ref[...].astype(F32), x)
    scale = lax.rsqrt(jnp.mean(x * x, axis=1, keepdims=True) + 0.5)
    norm_ref[...] = (x * scale * gain_ref[...]).astype(BF16)
    rows, width = out_ref.shape[0], norm_ref.shape[1] // 4
    expert, half, slot = row_codes(rows, x.shape[0])
    hit = by_expert(place_ref[...], expert) == slot.astype(F32)
    low = jnp.where(hit & (half == 0), 1.0, 0.0).astype(BF16)
    high = jnp.where(hit & (half == 1), 1.0, 0.0).astype(BF16)
    for part in range(2):
        got = jnp.dot(low, norm_ref[:, block(shift, part, width)], preferred_element_type=F32)
        got += jnp.dot(high, norm_ref[:, block(shift, part + 2, width)], preferred_element_type=F32)
        out_ref[:, part * width : (part + 1) * width] = got.astype(BF16)


def cot_kernel(meta, cot_ref, place_ref, share_ref, out_ref):
    shift = meta[0]
    rows, width = out_ref.shape[0], out_ref.shape[1] // 4
    expert, step, slot = row_codes(rows, cot_ref.shape[1])
    picks = []
    for k in range(2):
        hit = (by_expert(place_ref[k], expert) == slot.astype(F32)) & (step == k)
        picks.append(jnp.where(hit, by_expert(share_ref[k], expert), 0.0).astype(BF16))
    for part in range(4):
        got = jnp.dot(picks[0], cot_ref[0, :, block(shift, part, width)], preferred_element_type=F32)
        got += jnp.dot(picks[1], cot_ref[1, :, block(shift, part, width)], preferred_element_type=F32)
        out_ref[:, part * width : (part + 1) * width] = got.astype(BF16)


def expert_kernel(meta, x_ref, *refs):
    tops, bottoms = refs[0:4], refs[4:8]
    hidden_ref, keep_ref, send_ref = refs[8:11]
    core = meta[1]
    rows, width = x_ref.shape[0], tops[0].shape[1]
    hid = hidden_ref.shape[1]
    left, right = x_ref[:, :width], x_ref[:, width:]

    def project(weights):
        dot = functools.partial(lax.dot_general, dimension_numbers=NT, preferred_element_type=F32)
        low = dot(left, weights[0][:hid]) + dot(right, weights[1][:hid])
        high = dot(left, weights[2][:hid]) + dot(right, weights[3][:hid])
        half = (lax.broadcasted_iota(jnp.int32, low.shape, 0) // CAP) % 2
        both = jnp.where(half == 0, low, high)
        other = jnp.where(half == 0, pltpu.roll(both, rows - CAP, 0), pltpu.roll(both, CAP, 0))
        return both + other

    gate_act = project(tops)
    up_act = project(bottoms)
    hidden_ref[...] = (gate_act / (1.0 + jnp.exp(-gate_act)) * up_act).astype(BF16)
    mine = rows // 2
    for who, ref in ((1 - core, send_ref), (core, keep_ref)):
        h = hidden_ref[pl.ds(pl.multiple_of(who * mine, mine), mine), :]
        half = (lax.broadcasted_iota(jnp.int32, (mine, width), 0) // CAP) % 2
        for part in range(2):
            outs = []
            for k in (part, part + 2):
                down = jnp.concatenate([tops[k][hid:], bottoms[k][hid:]], axis=0)
                outs.append(jnp.dot(h, down, preferred_element_type=F32))
            ref[:, part * width : (part + 1) * width] = jnp.where(half == 0, outs[0], outs[1]).astype(BF16)


def grad_kernel(meta, first_ref, second_ref, own_ref, mate_ref, *refs):
    out_refs, mix_ref = refs[:4], refs[4]
    core = meta[1]
    rows = first_ref.shape[0]
    mine, width = rows // 2, out_refs[0].shape[1]
    step = (lax.broadcasted_iota(jnp.int32, first_ref.shape, 0) // CAP) % 2
    mix_ref[...] = jnp.where(step == 0, first_ref[...].astype(F32), second_ref[...].astype(F32)).astype(BF16)
    own = mix_ref[pl.ds(pl.multiple_of(core * mine, mine), mine), :]
    mate = mix_ref[pl.ds(pl.multiple_of((1 - core) * mine, mine), mine), :]
    for part in range(4):
        cols = slice(part * width, (part + 1) * width)
        got = lax.dot_general(own, own_ref[:, cols], TN, preferred_element_type=F32)
        got += lax.dot_general(mate, mate_ref[:, cols], TN, preferred_element_type=F32)
        out_refs[part][...] = got.astype(BF16)


def combine_kernel(use_second, meta, x_ref, y_ref, back_ref, place_ref, share_ref, *refs):
    shift = meta[0]
    out_ref = refs[-1]
    if use_second:
        out_ref[0] = refs[0][...]
    rows, width = back_ref.shape[0], back_ref.shape[1] // 2
    expert, half, slot = row_codes(rows, x_ref.shape[0])
    hit = by_expert(place_ref[...], expert) == slot.astype(F32)
    share = by_expert(share_ref[...], expert)
    mixes = [jnp.where(hit & (half == h), share, 0.0).astype(BF16) for h in range(2)]
    for part in range(4):
        cols = block(shift, part, width)
        x = x_ref[:, cols].astype(F32)
        if use_second:
            x = jnp.where(meta[2] == 1, y_ref[:, cols].astype(F32), x)
        at = (part % 2) * width
        got = lax.dot_general(mixes[part // 2], back_ref[:, at : at + width], TN, preferred_element_type=F32)
        result = (x + got).astype(BF16)
        if use_second:
            out_ref[1, :, cols] = result
        else:
            out_ref[:, cols] = result


def local(arrivals, fresh, routes, gates, cotangent, norm_gain, w_gate, w_up, w_down):
    n_expert, n_dp, n_section = lax.axis_size("expert"), lax.axis_size("dp"), lax.axis_size("section")
    chips = n_expert // 2
    flight = n_expert // SPLIT
    tokens, model_width = arrivals.shape[1], arrivals.shape[2]
    width = model_width // n_dp
    hid = w_gate.shape[1]
    rows = chips * 2 * CAP
    same_core = [[c + 2 * k for k in range(chips)] for c in range(2)]
    same_chip = [[2 * k, 2 * k + 1] for k in range(chips)]
    to_right = [(i, (i + 1) % n_dp) for i in range(n_dp)]
    to_left = [(i, (i - 1) % n_dp) for i in range(n_dp)]
    swap = [(i, i ^ 1) for i in range(n_expert)]
    meta = jnp.stack(
        [
            lax.axis_index("dp"),
            lax.axis_index("expert") % 2,
            (lax.axis_index("section") == 0).astype(jnp.int32),
        ]
    ).astype(jnp.int32)

    cut = hid // 2
    top = jnp.concatenate([w_gate[0], w_down[0, :cut]], axis=0)
    bottom = jnp.concatenate([w_up[0], w_down[0, cut:]], axis=0)
    top_3 = lax.ppermute(top, "dp", to_right)
    bottom_1 = lax.ppermute(bottom, "dp", to_left)
    bottom_3 = lax.ppermute(bottom, "dp", to_right)
    top_1 = lax.ppermute(top, "dp", to_left)
    top_2 = lax.ppermute(top_3, "dp", to_right)
    bottom_2 = lax.ppermute(bottom_1, "dp", to_left)
    weights = (top, top_1, top_2, top_3, bottom, bottom_1, bottom_2, bottom_3)

    routing = jnp.swapaxes(routes[0], 1, 2)
    shares = jnp.swapaxes(gates[0], 1, 2).astype(F32)
    matches = routing[:, None] == jnp.arange(flight, dtype=jnp.int32)[None, :, None, None]
    naming = jnp.any(matches, axis=2)
    share = jnp.sum(jnp.where(matches, shares[:, None], 0.0), axis=2)
    count = naming.astype(jnp.int32)
    place = jnp.where(naming, jnp.cumsum(count, axis=2) - count, 127).astype(F32)

    def exchange(packed):
        parts = packed.reshape(chips, 2 * CAP, packed.shape[1])
        got = lax.all_to_all(
            parts, "expert", split_axis=0, concat_axis=0, tiled=True, axis_index_groups=same_core
        )
        return got.reshape(packed.shape)

    def pack(x, y, k):
        return call(
            functools.partial(pack_kernel, k > 0),
            jax.ShapeDtypeStruct((rows, 2 * width), BF16),
            [pltpu.VMEM((tokens, model_width), BF16)],
            meta, x, y, norm_gain, place[k],
        )

    def run_experts(packed):
        both = lax.all_gather(
            exchange(packed), "expert", axis=0, tiled=True, axis_index_groups=same_chip
        )
        hidden, keep, send = call(
            expert_kernel,
            [
                jax.ShapeDtypeStruct((2 * rows, hid), BF16),
                jax.ShapeDtypeStruct((rows, 2 * width), BF16),
                jax.ShapeDtypeStruct((rows, 2 * width), BF16),
            ],
            [],
            meta, both, *weights,
        )
        received = lax.ppermute(send, "expert", swap)
        return hidden, (keep.astype(F32) + received.astype(F32)).astype(BF16)

    packed = pack(arrivals[0], arrivals[0], 0)
    cot_own = exchange(
        call(
            cot_kernel,
            jax.ShapeDtypeStruct((rows, model_width), BF16),
            [],
            meta, cotangent[0], place, share,
        )
    )
    hidden_0, summed = run_experts(packed)
    summed, cot_own = lax.optimization_barrier((summed, cot_own))
    cot_mate = lax.ppermute(cot_own, "expert", swap)
    out_0 = call(
        functools.partial(combine_kernel, False),
        jax.ShapeDtypeStruct((tokens, model_width), BF16),
        [],
        meta, arrivals[0], arrivals[0], exchange(summed), place[0], share[0],
    )
    shifted = lax.ppermute(out_0, "section", [(i, i + 1) for i in range(n_section - 1)])
    hidden_1, summed = run_experts(pack(shifted, fresh[0], 1))
    layer_out = call(
        functools.partial(combine_kernel, True),
        jax.ShapeDtypeStruct((2, tokens, model_width), BF16),
        [],
        meta, shifted, fresh[0], exchange(summed), place[1], share[1], out_0,
    )
    kept, right, far, left = call(
        grad_kernel,
        [jax.ShapeDtypeStruct((hid, width), BF16) for _ in range(n_dp)],
        [pltpu.VMEM((2 * rows, hid), BF16)],
        meta, hidden_0, hidden_1, cot_own, cot_mate,
    )
    across = [(i, (i + 2) % n_dp) for i in range(n_dp)]
    grad_part = kept.astype(F32)
    for part, pairs in ((far, across), (right, to_right), (left, to_left)):
        grad_part += lax.ppermute(part, "dp", pairs).astype(F32)
    return (layer_out[None], grad_part[None])


def solution(mesh):
    placed = (
        P("section", ("expert", "dp"), None),
        P(None, ("expert", "dp"), None),
        P("section", None, ("expert", "dp"), None),
        P("section", None, ("expert", "dp"), None),
        P("section", None, ("expert", "dp"), None),
        P("section", None),
        P("section", "expert", "dp"),
        P("section", "expert", "dp"),
        P("section", "expert", "dp"),
    )
    return jax.shard_map(
        local,
        mesh=mesh,
        in_specs=placed,
        out_specs=(P("section", None, ("expert", "dp"), None), P("section", "expert", "dp")),
        check_vma=False,
    )
```

```python
import functools

import jax
import jax.numpy as jnp
from jax import lax
from jax.experimental import pallas as pl
from jax.experimental.pallas import tpu as pltpu
from jax.sharding import PartitionSpec as P


SPLIT = 4
CAP = 12
VMEM = pltpu.MemorySpace.VMEM
F32 = jnp.float32
BF16 = jnp.bfloat16
NT = (((1,), (1,)), ((), ()))
TN = (((0,), (0,)), ((), ()))


def where():
    expert = lax.axis_index("expert")
    return lax.axis_index("dp"), expert % 2, lax.axis_index("section") == 0, (expert // 2) % 2


def call(body, outs, scratch, *args, vmem=12, far=(), raw=(), stay=(), own=False):
    n_in, n_out, n_scratch = len(args), len(outs), len(scratch)
    specs = [pl.BlockSpec(memory_space=pltpu.HBM if n in raw else VMEM) for n in range(n_in)]
    args = [pltpu.with_memory_space_constraint(a, pltpu.HBM) if n in stay else a for n, a in enumerate(args)]
    places = [pltpu.HBM if n in far else VMEM for n in range(n_out)]
    held = [args[n] for n in raw] + [outs[n] for n in far]
    staged = not own and bool(held)

    def kernel(*refs):
        refs = list(refs)
        spare = refs[n_in + n_out + n_scratch :]
        sems = spare[-1]
        copies = []
        for at, n in enumerate(raw):
            copies.append(pltpu.make_async_copy(refs[n], spare[at], sems.at[at]))
            copies[-1].start()
            refs[n] = spare[at]
        for copy in copies:
            copy.wait()
        copies = []
        for at, n in enumerate(far, len(raw)):
            copies.append(pltpu.make_async_copy(spare[at], refs[n_in + n], sems.at[at]))
            refs[n_in + n] = spare[at]
        body(where(), *refs[: n_in + n_out + n_scratch])
        for copy in copies:
            copy.start()
        for copy in copies:
            copy.wait()

    if staged:
        scratch = [*scratch, *(pltpu.VMEM(a.shape, a.dtype) for a in held), pltpu.SemaphoreType.DMA((len(held),))]
    got = pl.pallas_call(
        kernel if staged else lambda *refs: body(where(), *refs),
        out_shape=[pltpu.HBM(o.shape, o.dtype) if n in far else o for n, o in enumerate(outs)],
        in_specs=specs,
        out_specs=[pl.BlockSpec(memory_space=place) for place in places],
        scratch_shapes=scratch,
        compiler_params=pltpu.CompilerParams(vmem_limit_bytes=vmem * 1024 * 1024),
    )(*args)
    return got if len(got) > 1 else got[0]


def row_codes(rows, width):
    row = lax.broadcasted_iota(jnp.int32, (rows, width), 0)
    return row // (4 * CAP), (row // CAP) % 2, row % CAP


def by_expert(table, step, expert):
    out = table[6 + step : 7 + step, :]
    for e in (2, 1, 0):
        at = 2 * e + step
        out = jnp.where(expert == e, table[at : at + 1, :], out)
    return out


def block(shift, part, width):
    return pl.ds(pl.multiple_of(((shift + part) % 4) * width, width), width)


def fill_tables(route_ref, gate_ref, place_ref, share_ref):
    tokens = place_ref.shape[1]
    for e in range(place_ref.shape[0] // 2):
        named = jnp.zeros((2, tokens), F32)
        share = jnp.zeros((2, tokens), F32)
        for j in range(route_ref.shape[0]):
            hit = route_ref[j] == e
            named = jnp.where(hit, 1.0, named)
            share += jnp.where(hit, gate_ref[j].astype(F32), 0.0)
        place_ref[2 * e : 2 * e + 2, :] = named
        share_ref[2 * e : 2 * e + 2, :] = share
    named = place_ref[...]
    before = lax.broadcasted_iota(jnp.int32, (tokens, tokens), 0) < lax.broadcasted_iota(
        jnp.int32, (tokens, tokens), 1
    )
    count = jnp.dot(named.astype(BF16), jnp.where(before, 1.0, 0.0).astype(BF16), preferred_element_type=F32)
    place_ref[...] = jnp.where(named > 0.0, count, 127.0)


def copy_out(held, out_ref, sems, part, width):
    cols = pl.ds(part * width, width)
    return pltpu.make_async_copy(held.at[:, cols], out_ref.at[:, cols], sems.at[part])


def pack_kernel(k, meta, x_ref, gain_ref, *refs):
    shift = meta[0]
    x = x_ref[...].astype(F32)
    if k == 0:
        route_ref, gate_ref, out_ref, place_out, share_out, norm_ref, held, place_ref, share_ref, sems = refs
        fill_tables(route_ref, gate_ref, place_ref, share_ref)
        tables = [
            pltpu.make_async_copy(place_ref, place_out, sems.at[2]),
            pltpu.make_async_copy(share_ref, share_out, sems.at[3]),
        ]
    else:
        y_ref, place_in, out_ref, norm_ref, held, place_ref, sems = refs
        tables = [pltpu.make_async_copy(place_in, place_ref, sems.at[2])]
    for copy in tables:
        copy.start()
    if k == 1:
        x = jnp.where(meta[2], y_ref[...].astype(F32), x)
    scale = lax.rsqrt(jnp.mean(x * x, axis=1, keepdims=True) + 0.5)
    norm_ref[...] = (x * scale * gain_ref[...]).astype(BF16)
    rows, width = out_ref.shape[0], norm_ref.shape[1] // 4
    if k == 1:
        for copy in tables:
            copy.wait()
    expert, half, slot = row_codes(rows, x.shape[0])
    hit = by_expert(place_ref[...], k, expert) == slot.astype(F32)
    low = jnp.where(hit & (half == 0), 1.0, 0.0).astype(BF16)
    high = jnp.where(hit & (half == 1), 1.0, 0.0).astype(BF16)
    for part in range(2):
        got = jnp.dot(low, norm_ref[:, block(shift, part, width)], preferred_element_type=F32)
        got += jnp.dot(high, norm_ref[:, block(shift, part + 2, width)], preferred_element_type=F32)
        held[:, part * width : (part + 1) * width] = got.astype(BF16)
        copy_out(held, out_ref, sems, part, width).start()
    for part in range(2):
        copy_out(held, out_ref, sems, part, width).wait()
    if k == 0:
        for copy in tables:
            copy.wait()


def cot_kernel(meta, cot_ref, place_in, share_in, out_ref, held, place_ref, share_ref, sems):
    tables = [
        pltpu.make_async_copy(place_in, place_ref, sems.at[4]),
        pltpu.make_async_copy(share_in, share_ref, sems.at[5]),
    ]
    for copy in tables:
        copy.start()
    for copy in tables:
        copy.wait()
    shift = meta[0]
    rows, width = out_ref.shape[0], out_ref.shape[1] // 4
    row = lax.broadcasted_iota(jnp.int32, (rows, cot_ref.shape[1]), 0)
    expert, step, slot = row // (2 * CAP), (row // CAP) % 2, row % CAP
    picks = []
    for k in range(2):
        hit = (by_expert(place_ref[...], k, expert) == slot.astype(F32)) & (step == k)
        picks.append(jnp.where(hit, by_expert(share_ref[...], k, expert), 0.0).astype(BF16))
    for part in range(4):
        got = jnp.dot(picks[0], cot_ref[0, :, block(shift, part, width)], preferred_element_type=F32)
        got += jnp.dot(picks[1], cot_ref[1, :, block(shift, part, width)], preferred_element_type=F32)
        held[:, part * width : (part + 1) * width] = got.astype(BF16)
        copy_out(held, out_ref, sems, part, width).start()
    for part in range(4):
        copy_out(held, out_ref, sems, part, width).wait()


def split_steps_kernel(meta, own_ref, left_ref, right_ref, far_ref, out_ref):
    width, piece = out_ref.shape[1], out_ref.shape[0] // 8
    row = lax.broadcasted_iota(jnp.int32, (piece, 2 * piece), 0)
    col = lax.broadcasted_iota(jnp.int32, (piece, 2 * piece), 1)
    source = (row // CAP) * (2 * CAP) + row % CAP
    for step in range(2):
        take = jnp.where(col == source + step * CAP, 1.0, 0.0).astype(BF16)
        for n, ref in enumerate((own_ref, left_ref, right_ref, far_ref)):
            at = (step * 4 + n) * piece
            got = jnp.dot(take, ref[:, :width], preferred_element_type=F32)
            out_ref[at : at + piece, :] = got.astype(BF16)


def expert_kernel(meta, x_ref, *refs):
    raw, (slots_ref, keep_ref, send_ref), scratch = refs[:8], refs[8:11], refs[11:]
    held, (halves, outs, hidden_ref, sems) = scratch[:8], scratch[8:]
    copies = [pltpu.make_async_copy(raw[n], held[n], sems.at[n]) for n in range(8)]
    for copy in copies:
        copy.start()
    core = meta[1]
    mine, width = x_ref.shape[0] // 2, held[0].shape[1]
    slots, hid = hidden_ref.shape[0] // 2, hidden_ref.shape[1]
    row = lax.broadcasted_iota(jnp.int32, (slots, mine), 0)
    col = lax.broadcasted_iota(jnp.int32, (slots, mine), 1)
    source = (2 * ((row // CAP) % 4) + row // (4 * CAP)) * (2 * CAP) + row % CAP
    for h in range(2):
        take = jnp.where(col == source + h * CAP, 1.0, 0.0).astype(BF16)
        for c in range(2):
            got = jnp.dot(take, x_ref[c * mine : (c + 1) * mine, :], preferred_element_type=F32)
            halves[h, c * slots : (c + 1) * slots, :] = got.astype(BF16)

    def project(first):
        total = 0.0
        for k in range(4):
            copies[first + k].wait()
            rows = halves[k // 2, :, (k % 2) * width : (k % 2 + 1) * width]
            total += lax.dot_general(rows, held[first + k][:hid, :], NT, preferred_element_type=F32)
        return total

    gate_act = project(0)
    up_act = project(4)
    hidden = (gate_act / (1.0 + jnp.exp(-gate_act)) * up_act).astype(BF16)
    hidden_ref[...] = hidden
    keep_hidden = pltpu.make_async_copy(hidden_ref, slots_ref, sems.at[8])
    keep_hidden.start()
    for k in range(4):
        down = jnp.concatenate([held[k][hid:, :], held[4 + k][hid:, :]], axis=0)
        outs[k] = jnp.dot(hidden, down, preferred_element_type=F32).astype(BF16)
    row = lax.broadcasted_iota(jnp.int32, (mine, slots), 0)
    col = lax.broadcasted_iota(jnp.int32, (mine, slots), 1)
    chip, half = row // (2 * CAP), (row // CAP) % 2
    found = col == (chip % 2) * (4 * CAP) + (chip // 2) * CAP + row % CAP
    puts = [jnp.where(found & (half == h), 1.0, 0.0).astype(BF16) for h in range(2)]
    for who, ref in ((1 - core, send_ref), (core, keep_ref)):
        from_rows = pl.ds(pl.multiple_of(who * slots, slots), slots)
        for part in range(2):
            got = jnp.dot(puts[0], outs[part, from_rows, :], preferred_element_type=F32)
            got += jnp.dot(puts[1], outs[part + 2, from_rows, :], preferred_element_type=F32)
            ref[:, part * width : (part + 1) * width] = got.astype(BF16)
    keep_hidden.wait()


def first_grad_kernel(meta, own_ref, chip_ref, mate_ref, far_ref, *refs):
    hiddens, (late_ref, out_ref, early_ref) = refs[:4], refs[4:]
    core, half = meta[1], meta[3]
    piece = own_ref.shape[0] // 8
    for at, ref in (
        (core * 2 + half, own_ref),
        (core * 2 + 1 - half, chip_ref),
        ((1 - core) * 2 + half, mate_ref),
        ((1 - core) * 2 + 1 - half, far_ref),
    ):
        for n in range(4):
            to = pl.ds(pl.multiple_of((n * 4 + at) * piece, piece), piece)
            early_ref[to, :] = ref[n * piece : (n + 1) * piece, :]
            late_ref[to, :] = ref[(4 + n) * piece : (5 + n) * piece, :]
    out_ref[...] = slot_grads(hiddens, early_ref)


def slot_grads(hiddens, cot_ref):
    total = 0.0
    for n, ref in enumerate(hiddens):
        slots = ref.shape[0]
        total += lax.dot_general(ref[...], cot_ref[n * slots : (n + 1) * slots, :], TN, preferred_element_type=F32)
    return total


def second_grad_kernel(meta, first_ref, cot_ref, *refs):
    refs[4][...] = first_ref[...] + slot_grads(refs[:4], cot_ref)


def combine_kernel(k, meta, x_ref, y_ref, back_ref, place_ref, share_ref, *refs):
    shift = meta[0]
    out_ref = refs[-1]
    if k:
        out_ref[0] = refs[0][...]
    rows, width = back_ref.shape[0], back_ref.shape[1] // 2
    expert, half, slot = row_codes(rows, x_ref.shape[0])
    hit = by_expert(place_ref[...], k, expert) == slot.astype(F32)
    share = by_expert(share_ref[...], k, expert)
    mixes = [jnp.where(hit & (half == h), share, 0.0).astype(BF16) for h in range(2)]
    for part in range(4):
        cols = block(shift, part, width)
        x = x_ref[:, cols].astype(F32)
        if k:
            x = jnp.where(meta[2], y_ref[:, cols].astype(F32), x)
        at = (part % 2) * width
        got = lax.dot_general(mixes[part // 2], back_ref[:, at : at + width], TN, preferred_element_type=F32)
        result = (x + got).astype(BF16)
        if k:
            out_ref[1, :, cols] = result
        else:
            out_ref[:, cols] = result


def program(arrivals, fresh, routes, gates, cotangent, norm_gain, w_gate, w_up, w_down):
    n_expert, n_dp, n_section = lax.axis_size("expert"), lax.axis_size("dp"), lax.axis_size("section")
    chips = n_expert // 2
    flight = n_expert // SPLIT
    tokens, model_width = arrivals.shape[1], arrivals.shape[2]
    width = model_width // n_dp
    hid = w_gate.shape[1]
    rows = chips * 2 * CAP
    same_core = [[c + 2 * k for k in range(chips)] for c in range(2)]
    same_place = [[p + SPLIT * e for e in range(flight)] for p in range(SPLIT)]
    same_chip = [[2 * k, 2 * k + 1] for k in range(chips)]
    to_right = [(i, (i + 1) % n_dp) for i in range(n_dp)]
    to_left = [(i, (i - 1) % n_dp) for i in range(n_dp)]
    across = [(i, (i + 2) % n_dp) for i in range(n_dp)]
    other_chip = [(i, i ^ 2) for i in range(n_expert)]
    swap = [(i, i ^ 1) for i in range(n_expert)]
    core = lax.axis_index("expert") % 2

    cut = hid // 2
    top = jnp.concatenate([w_gate[0], w_down[0, :cut]], axis=0)
    bottom = jnp.concatenate([w_up[0], w_down[0, cut:]], axis=0)
    top_3 = lax.ppermute(top, "dp", to_right)
    bottom_1 = lax.ppermute(bottom, "dp", to_left)
    bottom_3 = lax.ppermute(bottom, "dp", to_right)
    top_1 = lax.ppermute(top, "dp", to_left)
    top_2 = lax.ppermute(top_3, "dp", to_right)
    bottom_2 = lax.ppermute(bottom_1, "dp", to_left)
    weights = (top, top_1, top_2, top_3, bottom, bottom_1, bottom_2, bottom_3)

    def exchange(packed):
        parts = packed.reshape(chips, 2 * CAP, packed.shape[1])
        got = lax.all_to_all(
            parts, "expert", split_axis=0, concat_axis=0, tiled=True, axis_index_groups=same_core
        )
        return got.reshape(packed.shape)

    def both_cores(rows_in):
        return lax.all_gather(rows_in, "expert", axis=0, tiled=True, axis_index_groups=same_chip)

    packed_rows = jax.ShapeDtypeStruct((rows, 2 * width), BF16)
    norm_scratch = [
        pltpu.VMEM((tokens, model_width), BF16),
        pltpu.VMEM((rows, 2 * width), BF16),
    ]
    table = jax.ShapeDtypeStruct((2 * flight, tokens), F32)
    table_scratch = pltpu.VMEM(table.shape, F32)

    def run_experts(received):
        received = both_cores(received)
        hidden, keep, send = call(
            expert_kernel,
            [jax.ShapeDtypeStruct((rows, hid), BF16), packed_rows, packed_rows],
            [
                *(pltpu.VMEM((hid + cut, width), BF16) for _ in range(8)),
                pltpu.VMEM((2, rows, 2 * width), BF16),
                pltpu.VMEM((4, rows, width), BF16),
                pltpu.VMEM((rows, hid), BF16),
                pltpu.SemaphoreType.DMA((9,)),
            ],
            received, *weights,
            vmem=20,
            raw=range(1, 9), far=(0,), own=True,
        )
        sent = lax.dynamic_slice_in_dim(both_cores(send), (1 - core) * rows, rows, 0)
        return hidden, (keep.astype(F32) + sent.astype(F32)).astype(BF16)

    packed, place, share = call(
        functools.partial(pack_kernel, 0),
        [packed_rows, table, table],
        [*norm_scratch, table_scratch, table_scratch, pltpu.SemaphoreType.DMA((4,))],
        arrivals[0], norm_gain,
        jnp.transpose(routes[0], (2, 0, 1)), jnp.transpose(gates[0], (2, 0, 1)),
        far=(0, 1, 2), own=True,
    )
    received = exchange(packed)
    packed_cot = call(
        cot_kernel,
        [jax.ShapeDtypeStruct((rows // 2, model_width), BF16)],
        [
            pltpu.VMEM((rows // 2, model_width), BF16),
            table_scratch,
            table_scratch,
            pltpu.SemaphoreType.DMA((6,)),
        ],
        cotangent[0], place, share,
        raw=(1, 2), stay=(1, 2), far=(0,), own=True,
    )
    cot_rows = lax.all_to_all(
        packed_cot.reshape(flight, 2 * CAP, model_width),
        "expert", split_axis=0, concat_axis=0, tiled=True, axis_index_groups=same_place,
    ).reshape(rows // 2, model_width)
    hidden_0, summed = run_experts(received)
    summed, cot_rows = lax.optimization_barrier((summed, cot_rows))
    back = exchange(summed)

    def to_dp(parts):
        moved = []
        for part, pairs in ((parts[1], across), (parts[0], to_right), (parts[2], to_left)):
            moved.append(lax.ppermute(part, "dp", pairs))
        return moved[1:] + moved[:1]

    columns = [cot_rows[:, n * width : (n + 1) * width] for n in range(1, 4)]
    pieces = to_dp(columns)
    cot_own = call(
        split_steps_kernel,
        [jax.ShapeDtypeStruct((2 * rows, width), BF16)],
        [],
        cot_rows, *pieces,
        raw=range(4), far=(0,),
    )
    cot_chip = lax.ppermute(cot_own, "expert", other_chip)
    cot_mate = lax.ppermute(cot_own, "expert", swap)
    cot_last = lax.ppermute(cot_chip, "expert", swap)
    grad = jax.ShapeDtypeStruct((hid, width), F32)
    others = to_dp([hidden_0] * 3)
    cot_late, grad_0 = call(
        first_grad_kernel,
        [jax.ShapeDtypeStruct((4 * rows, width), BF16), grad],
        [pltpu.VMEM((4 * rows, width), BF16)],
        cot_own, cot_chip, cot_mate, cot_last, hidden_0, *others,
        raw=range(8), far=(0, 1), stay=(0, 4),
    )

    out_0 = call(
        functools.partial(combine_kernel, 0),
        [jax.ShapeDtypeStruct((tokens, model_width), BF16)],
        [],
        arrivals[0], arrivals[0], back, place, share,
        raw=(0, 2, 3, 4), stay=(0, 3, 4),
    )
    shifted = lax.ppermute(out_0, "section", [(i, i + 1) for i in range(n_section - 1)])
    packed = call(
        functools.partial(pack_kernel, 1),
        [packed_rows],
        [*norm_scratch, table_scratch, pltpu.SemaphoreType.DMA((3,))],
        shifted, norm_gain, fresh[0], place,
        raw=(3,), stay=(3,), far=(0,), own=True,
    )
    received = exchange(packed)
    hidden_1, summed = run_experts(received)
    back = exchange(summed)
    layer_out = call(
        functools.partial(combine_kernel, 1),
        [jax.ShapeDtypeStruct((2, tokens, model_width), BF16)],
        [],
        shifted, fresh[0], back, place, share, out_0,
        raw=range(6), stay=(1, 3, 4),
    )
    others = to_dp([hidden_1] * 3)
    grad_part = call(second_grad_kernel, [grad], [], grad_0, cot_late, hidden_1, *others, raw=range(6), stay=range(3))
    return (layer_out[None], grad_part[None])


def solution(mesh):
    placed = (
        P("section", ("expert", "dp"), None),
        P(None, ("expert", "dp"), None),
        P("section", None, ("expert", "dp"), None),
        P("section", None, ("expert", "dp"), None),
        P("section", None, ("expert", "dp"), None),
        P("section", None),
        P("section", "expert", "dp"),
        P("section", "expert", "dp"),
        P("section", "expert", "dp"),
    )
    return jax.shard_map(
        program,
        mesh=mesh,
        in_specs=placed,
        out_specs=(P("section", None, ("expert", "dp"), None), P("section", "expert", "dp")),
        check_vma=False,
    )
```
